32 devices in a mesh: data: 32 (over z, y, x, core).
Axes of the slice: x: 2, y: 2, z: 4, core: 2. Of those that a mesh axis runs over, the one named last changes fastest.
Arguments:
- feat_a: bfloat16 [2048, 2048], P('data')
- feat_b: bfloat16 [2048, 2048], P('data')
- w_one: bfloat16 [2048, 2048], replicated
- w_two: bfloat16 [2048, 2048], replicated
- w_three: bfloat16 [2048, 2048], replicated
- g_one: float32 [2048], replicated
- b_one: float32 [2048], replicated
- g_two: float32 [2048], replicated
- b_two: float32 [2048], replicated
- lam_off: float32 [], replicated
Outputs:
- output 1: float32 [], replicated
- output 2: float32 [2048, 2048], replicated
- output 3: float32 [2048, 2048], replicated
- output 4: float32 [2048, 2048], replicated
- output 5: float32 [2048], replicated
- output 6: float32 [2048], replicated
- output 7: float32 [2048], replicated
- output 8: float32 [2048], replicated
All inputs are finite; a program needn't handle non-finite values.
Results may differ from the reference program's by a relative error of at most 0.00637.
Values are sent between devices in bfloat16 or wider.
A program may use at most 1 GiB of HBM per device.

```python
import jax
import jax.numpy as jnp
from jax import lax

F = 2048
D = 2048
ROWS_DEV = 64
DATA_DEVS = 32
ROWS_ALL = ROWS_DEV * DATA_DEVS
NORM_EPS = 1e-5


def setup_inputs(seed: int = 0) -> dict:
    key_list = jax.random.split(jax.random.key(seed), 13)
    common = jax.random.normal(key_list[0], (ROWS_ALL, F), jnp.float32)
    offset = 0.8 * jax.random.normal(key_list[3], (DATA_DEVS, 1, F), jnp.float32)
    spread = jax.random.uniform(key_list[4], (DATA_DEVS, 1, F), jnp.float32, 0.5, 1.5)

    def shard_shift(values):
        return (values.reshape(DATA_DEVS, ROWS_DEV, F) * spread + offset).reshape(ROWS_ALL, F)

    noise_a = jax.random.normal(key_list[1], (ROWS_ALL, F), jnp.float32)
    noise_b = jax.random.normal(key_list[2], (ROWS_ALL, F), jnp.float32)
    feat_a = shard_shift(common + 0.65 * noise_a)
    feat_b = shard_shift(common + 0.65 * noise_b)
    w_one = jax.random.normal(key_list[5], (F, D), jnp.float32) * F ** -0.5
    w_two = jax.random.normal(key_list[6], (D, D), jnp.float32) * D ** -0.5
    w_three = jax.random.normal(key_list[7], (D, D), jnp.float32) * D ** -0.5
    g_one = jax.random.uniform(key_list[8], (D,), jnp.float32, 0.5, 1.5)
    b_one = 0.5 * jax.random.normal(key_list[9], (D,), jnp.float32)
    g_two = jax.random.uniform(key_list[10], (D,), jnp.float32, 0.5, 1.5)
    b_two = 0.5 * jax.random.normal(key_list[11], (D,), jnp.float32)
    lam_off = jax.random.uniform(key_list[12], (), jnp.float32, 0.15, 0.45) * ROWS_ALL / D
    return {'feat_a': feat_a.astype(jnp.bfloat16), 'feat_b': feat_b.astype(jnp.bfloat16), 'w_one': w_one.astype(jnp.bfloat16), 'w_two': w_two.astype(jnp.bfloat16), 'w_three': w_three.astype(jnp.bfloat16), 'g_one': g_one, 'b_one': b_one, 'g_two': g_two, 'b_two': b_two, 'lam_off': lam_off}


def normalize(pre):
    mean_val = jnp.mean(pre, axis=0)
    var_val = jnp.mean(pre * pre, axis=0) - mean_val * mean_val
    inv_std = lax.rsqrt(var_val + NORM_EPS)
    return (pre - mean_val) * inv_std, inv_std


def normalize_back(grad_norm, normed, inv_std):
    centred = grad_norm - jnp.mean(grad_norm, axis=0)
    return inv_std * (centred - normed * jnp.mean(grad_norm * normed, axis=0))


def forward_view(feat, w_one, w_two, w_three, g_one, b_one, g_two, b_two):
    pre_one = jnp.dot(feat, w_one, preferred_element_type=jnp.float32)
    norm_one, inv_one = normalize(pre_one)
    aff_one = norm_one * g_one + b_one
    act_one = jnp.maximum(aff_one, 0.0).astype(jnp.bfloat16)
    pre_two = jnp.dot(act_one, w_two, preferred_element_type=jnp.float32)
    norm_two, inv_two = normalize(pre_two)
    aff_two = norm_two * g_two + b_two
    act_two = jnp.maximum(aff_two, 0.0).astype(jnp.bfloat16)
    proj_out = jnp.dot(act_two, w_three, preferred_element_type=jnp.float32)
    norm_out, inv_out = normalize(proj_out)
    return (act_one, act_two, norm_one, norm_two, aff_one, aff_two, norm_out, inv_one, inv_two, inv_out)


def backward_view(feat, grad_emb, saved, w_two, w_three, g_one, g_two):
    act_one, act_two, norm_one, norm_two, aff_one, aff_two, norm_out, inv_one, inv_two, inv_out = saved
    grad_proj = normalize_back(grad_emb, norm_out, inv_out).astype(jnp.bfloat16)
    dw_three = jnp.dot(act_two.T, grad_proj, preferred_element_type=jnp.float32)
    grad_act_two = jnp.dot(grad_proj, w_three.T, preferred_element_type=jnp.float32)
    grad_aff_two = jnp.where(aff_two > 0, grad_act_two, 0.0)
    dg_two = jnp.sum(grad_aff_two * norm_two, axis=0)
    db_two = jnp.sum(grad_aff_two, axis=0)
    grad_pre_two = normalize_back(grad_aff_two * g_two, norm_two, inv_two).astype(jnp.bfloat16)
    dw_two = jnp.dot(act_one.T, grad_pre_two, preferred_element_type=jnp.float32)
    grad_act_one = jnp.dot(grad_pre_two, w_two.T, preferred_element_type=jnp.float32)
    grad_aff_one = jnp.where(aff_one > 0, grad_act_one, 0.0)
    dg_one = jnp.sum(grad_aff_one * norm_one, axis=0)
    db_one = jnp.sum(grad_aff_one, axis=0)
    grad_pre_one = normalize_back(grad_aff_one * g_one, norm_one, inv_one).astype(jnp.bfloat16)
    dw_one = jnp.dot(feat.T, grad_pre_one, preferred_element_type=jnp.float32)
    return (dw_one, dw_two, dw_three, dg_one, db_one, dg_two, db_two)


def reference(feat_a, feat_b, w_one, w_two, w_three, g_one, b_one, g_two, b_two, lam_off):
    saved_a = forward_view(feat_a, w_one, w_two, w_three, g_one, b_one, g_two, b_two)
    saved_b = forward_view(feat_b, w_one, w_two, w_three, g_one, b_one, g_two, b_two)
    emb_a = saved_a[6].astype(jnp.bfloat16)
    emb_b = saved_b[6].astype(jnp.bfloat16)
    corr = jnp.dot(emb_a.T, emb_b, preferred_element_type=jnp.float32) / ROWS_ALL
    diag_c = jnp.diagonal(corr)
    loss_val = jnp.sum((1.0 - diag_c) ** 2) + lam_off * (jnp.sum(corr * corr) - jnp.sum(diag_c * diag_c))
    on_diag = jnp.arange(D)[:, None] == jnp.arange(D)[None, :]
    grad_c = jnp.where(on_diag, -2.0 * (1.0 - corr), 2.0 * lam_off * corr).astype(jnp.bfloat16)
    grad_a = jnp.dot(emb_b, grad_c.T, preferred_element_type=jnp.float32) / ROWS_ALL
    grad_b = jnp.dot(emb_a, grad_c, preferred_element_type=jnp.float32) / ROWS_ALL
    grads_a = backward_view(feat_a, grad_a, saved_a, w_two, w_three, g_one, g_two)
    grads_b = backward_view(feat_b, grad_b, saved_b, w_two, w_three, g_one, g_two)
    return (loss_val, grads_a[0] + grads_b[0], grads_a[1] + grads_b[1], grads_a[2] + grads_b[2], grads_a[3] + grads_b[3], grads_a[4] + grads_b[4], grads_a[5] + grads_b[5], grads_a[6] + grads_b[6])
```

```python
import jax
import jax.numpy as jnp
from jax import lax
from jax.sharding import PartitionSpec as P

NORM_EPS = 1e-5
BATCH_AXIS = 'data'


def stats(pre):
    mean_val = jnp.mean(pre, axis=0)
    var_val = jnp.mean(pre * pre, axis=0) - mean_val * mean_val
    return mean_val, lax.rsqrt(var_val + NORM_EPS)


def norm_back(grad_norm, normed, inv_std):
    mean_grad = jnp.mean(grad_norm, axis=0)
    mean_cross = jnp.mean(grad_norm * normed, axis=0)
    return inv_std * (grad_norm - mean_grad - normed * mean_cross)


def dot(lhs, rhs, lhs_dim, rhs_dim):
    return lax.dot_general(lhs, rhs, (((lhs_dim,), (rhs_dim,)), ((), ())), preferred_element_type=jnp.float32)


def solution(mesh):
    num_devs = mesh.shape[BATCH_AXIS]
    swap = [(i, i ^ 1) for i in range(num_devs)]
    same_core = [list(range(k, num_devs, 2)) for k in range(2)]

    def exchange(val):
        return lax.ppermute(val, BATCH_AXIS, swap)

    def local_step(feat_a, feat_b, w_one, w_two, w_three, g_one, b_one, g_two, b_two, lam_off):
        rows_all = feat_a.shape[0] * num_devs
        width = w_two.shape[0]
        first = (lax.axis_index(BATCH_AXIS) % 2) == 0
        mine = jnp.where(first, feat_a, feat_b)
        got = exchange(jnp.where(first, feat_b, feat_a))
        rows = jnp.where(first, jnp.concatenate([mine, got]), jnp.concatenate([got, mine]))
        feat = lax.all_gather(rows, BATCH_AXIS, axis_index_groups=same_core, tiled=True)
        pre_one = dot(feat, w_one, 1, 0)
        mean_one, inv_one = stats(pre_one)
        norm_one = (pre_one - mean_one) * inv_one
        aff_one = norm_one * g_one + b_one
        act_one = jnp.maximum(aff_one, 0.0).astype(jnp.bfloat16)
        pre_two = dot(act_one, w_two, 1, 0)
        mean_two, inv_two = stats(pre_two)
        norm_two = (pre_two - mean_two) * inv_two
        aff_two = norm_two * g_two + b_two
        act_two = jnp.maximum(aff_two, 0.0).astype(jnp.bfloat16)
        proj_out = dot(act_two, w_three, 1, 0)
        mean_out, inv_out = stats(proj_out)
        norm_out = (proj_out - mean_out) * inv_out
        emb = norm_out.astype(jnp.bfloat16)
        other = exchange(emb)
        corr = dot(emb, other, 0, 0) / rows_all
        on_diag = jnp.arange(width)[:, None] == jnp.arange(width)[None, :]
        loss_val = jnp.sum(jnp.where(on_diag, (1.0 - corr) ** 2, lam_off * corr * corr))
        grad_c = jnp.where(on_diag, -2.0 * (1.0 - corr), 2.0 * lam_off * corr).astype(jnp.bfloat16)
        loss_val = jnp.where(first, loss_val, 0.0)
        grad_emb = dot(other, grad_c, 1, 1) / rows_all
        grad_proj = norm_back(grad_emb, norm_out, inv_out).astype(jnp.bfloat16)
        part_three = dot(act_two, grad_proj, 0, 0)
        grad_act_two = dot(grad_proj, w_three, 1, 1)
        grad_aff_two = jnp.where(aff_two > 0, grad_act_two, 0.0)
        dg_two = jnp.sum(grad_aff_two * norm_two, axis=0)
        db_two = jnp.sum(grad_aff_two, axis=0)
        grad_pre_two = norm_back(grad_aff_two * g_two, norm_two, inv_two).astype(jnp.bfloat16)
        part_two = dot(act_one, grad_pre_two, 0, 0)
        grad_act_one = dot(grad_pre_two, w_two, 1, 1)
        grad_aff_one = jnp.where(aff_one > 0, grad_act_one, 0.0)
        dg_one = jnp.sum(grad_aff_one * norm_one, axis=0)
        db_one = jnp.sum(grad_aff_one, axis=0)
        grad_pre_one = norm_back(grad_aff_one * g_one, norm_one, inv_one).astype(jnp.bfloat16)
        part_one = dot(feat, grad_pre_one, 0, 0)
        dw_three = part_three + exchange(part_three)
        dw_two = part_two + exchange(part_two)
        dw_one = part_one + exchange(part_one)
        small = jnp.stack([dg_one, db_one, dg_two, db_two, jnp.full((width,), loss_val)])
        small = small + exchange(small)
        return (small[4, 0], dw_one, dw_two, dw_three, small[0], small[1], small[2], small[3])

    row_spec = P(BATCH_AXIS, None)
    return jax.shard_map(local_step, mesh=mesh, in_specs=(row_spec, row_spec, P(), P(), P(), P(), P(), P(), P(), P()), out_specs=(P(), P(), P(), P(), P(), P(), P(), P()), check_vma=False)
```

```python
import functools

import jax
import jax.numpy as jnp
from jax import lax
from jax.experimental import pallas as pl
from jax.experimental.pallas import tpu as pltpu
from jax.sharding import PartitionSpec as P

NORM_EPS = 1e-5
BATCH_AXIS = 'data'
MESH_ID = pl.DeviceIdType.MESH
TILE = 256
CHUNK = 512
BF = jnp.bfloat16
F32 = jnp.float32


def mm(lhs, rhs, lhs_dim=1, rhs_dim=0):
    return lax.dot_general(lhs, rhs, (((lhs_dim,), (rhs_dim,)), ((), ())), preferred_element_type=F32)


def fold(val):
    return jnp.sum(val.reshape(val.shape[0] // 8, 8, val.shape[1]), axis=0)


def sibling_of(me):
    return me + 1 - 2 * lax.rem(me, 2)


def greet(peers):
    barrier = pltpu.get_barrier_semaphore()
    for peer in peers:
        pl.semaphore_signal(barrier, inc=1, device_id=(peer,), device_id_type=MESH_ID)
    pl.semaphore_wait(barrier, len(peers))


def remote(src, dst, send_sem, recv_sem, dev):
    return pltpu.make_async_remote_copy(src_ref=src, dst_ref=dst, send_sem=send_sem, recv_sem=recv_sem, device_id=(dev,), device_id_type=MESH_ID)


def gather_kernel(rows, own_ref, out_ref, buf, own_sem, sib_s, sib_r, send_sem, recv_sem, half_s, half_r, out_sem):
    me = lax.axis_index(BATCH_AXIS)
    core = lax.rem(me, 2)
    sib = sibling_of(me)
    chip = me // 2
    xpos = lax.rem(chip, 2)
    ypos = lax.rem(chip // 2, 2)
    zpos = chip // 4
    x_dev = me + 2 - 4 * xpos
    y_dev = me + 4 - 8 * ypos
    up_dev = jnp.minimum(zpos + 1, 3) * 8 + lax.rem(me, 8)
    down_dev = jnp.maximum(zpos - 1, 0) * 8 + lax.rem(me, 8)
    barrier = pltpu.get_barrier_semaphore()
    for peer in (sib, x_dev, y_dev):
        pl.semaphore_signal(barrier, inc=1, device_id=(peer,), device_id_type=MESH_ID)
    has_up = zpos < 3
    has_down = zpos > 0

    @pl.when(has_up)
    def _():
        pl.semaphore_signal(barrier, inc=1, device_id=(up_dev,), device_id_type=MESH_ID)

    @pl.when(has_down)
    def _():
        pl.semaphore_signal(barrier, inc=1, device_id=(down_dev,), device_id_type=MESH_ID)
    pl.semaphore_wait(barrier, 3 + (1 - (zpos + 1) // 4) + (zpos + 3) // 4)

    def block(idx):
        return buf.at[pl.ds(pl.multiple_of(idx * 2 * rows, 2 * rows), 2 * rows), :]

    def half(idx, part):
        return buf.at[pl.ds(pl.multiple_of(idx * 2 * rows + part * rows, rows), rows), :]

    own = pltpu.make_async_copy(own_ref.at[core], half(chip, core), own_sem)
    own.start()
    to_sib = remote(own_ref.at[1 - core], half(chip, core), sib_s, sib_r, sib)
    to_sib.start()
    own.wait()
    to_sib.wait()

    def whole(idx, way, dev):
        return remote(block(idx), block(idx), send_sem.at[idx, way], recv_sem.at[idx], dev)

    def part_copy(idx, part, dev):
        return remote(half(idx, part), half(idx, part), half_s.at[idx], half_r.at[idx, part], dev)

    def blk(xx, yy, zz):
        return (zz * 2 + yy) * 2 + xx

    def column(zz, going_up, going_down):
        idx = blk(xpos, ypos, zz)
        whole(idx, 0, x_dev).start()
        whole(idx, 1, y_dev).start()
        if going_up:
            @pl.when(has_up)
            def _():
                whole(idx, 2, up_dev).start()
        if going_down:
            @pl.when(has_down)
            def _():
                whole(idx, 3, down_dev).start()

    def across(zz):
        idx_x = blk(1 - xpos, ypos, zz)
        whole(idx_x, 0, x_dev).wait_recv()
        part_copy(idx_x, 0, y_dev).start()
        idx_y = blk(xpos, 1 - ypos, zz)
        whole(idx_y, 1, y_dev).wait_recv()
        part_copy(idx_y, 1, x_dev).start()

    column(zpos, True, True)
    for dist in range(1, 5):
        for sign in (-1, 1):
            zz = zpos + sign * dist
            if dist < 4:
                @pl.when(jnp.logical_and(zz >= 0, zz < 4))
                def _(zz=zz, sign=sign):
                    whole(blk(xpos, ypos, zz), 0, x_dev).wait_recv()
                    column(zz, sign < 0, sign > 0)
            prev = zpos + sign * (dist - 1)
            if dist > 1 or sign < 0:
                @pl.when(jnp.logical_and(prev >= 0, prev < 4))
                def _(prev=prev):
                    across(prev)
    def finish(zz, carry):
        idx = blk(1 - xpos, 1 - ypos, zz)
        part_copy(idx, 0, y_dev).wait_recv()
        part_copy(idx, 1, x_dev).wait_recv()
        return carry
    lax.fori_loop(0, 4, finish, 0)
    out = pltpu.make_async_copy(buf, out_ref, out_sem)
    out.start()

    def drain(zz, carry):
        col = blk(xpos, ypos, zz)
        whole(col, 0, x_dev).wait_send()
        whole(col, 1, y_dev).wait_send()

        @pl.when(jnp.logical_and(has_up, zz <= zpos))
        def _():
            whole(col, 2, up_dev).wait_send()

        @pl.when(jnp.logical_and(has_down, zz >= zpos))
        def _():
            whole(col, 3, down_dev).wait_send()
        part_copy(blk(1 - xpos, ypos, zz), 0, y_dev).wait_send()
        part_copy(blk(xpos, 1 - ypos, zz), 1, x_dev).wait_send()
        return carry
    lax.fori_loop(0, 4, drain, 0)
    out.wait()


def gather_rows(own, num_devs):
    rows, width = own.shape[1:]
    chips = num_devs // 2
    return pl.pallas_call(
        functools.partial(gather_kernel, rows),
        out_shape=jax.ShapeDtypeStruct((num_devs * rows, width), own.dtype),
        in_specs=[pl.BlockSpec(memory_space=pltpu.VMEM)],
        out_specs=pl.BlockSpec(memory_space=pl.ANY),
        scratch_shapes=[pltpu.VMEM((num_devs * rows, width), own.dtype), pltpu.SemaphoreType.DMA, pltpu.SemaphoreType.DMA, pltpu.SemaphoreType.DMA,
                        pltpu.SemaphoreType.DMA((chips, 4)), pltpu.SemaphoreType.DMA((chips,)),
                        pltpu.SemaphoreType.DMA((chips,)), pltpu.SemaphoreType.DMA((chips, 2)), pltpu.SemaphoreType.DMA],
        compiler_params=pltpu.CompilerParams(collective_id=0, has_side_effects=True, vmem_limit_bytes=60 << 20),
        name='gather_rows',
    )(own)


def pre_stats(x_ref, w, pre_ref):
    rows = x_ref.shape[0]

    def step(i, carry):
        at = pl.ds(pl.multiple_of(i * CHUNK, CHUNK), CHUNK)
        val = mm(x_ref[at, :], w)
        pre_ref[at, :] = val
        return carry[0] + fold(val), carry[1] + fold(val * val)
    zero = jnp.zeros((8, pre_ref.shape[1]), F32)
    tot, sqr = lax.fori_loop(0, rows // CHUNK, step, (zero, zero), unroll=True)
    mean = jnp.sum(tot, axis=0, keepdims=True) / rows
    var = jnp.sum(sqr, axis=0, keepdims=True) / rows - mean * mean
    return mean, lax.rsqrt(var + NORM_EPS)


def layer_kernel(x_ref, w_ref, g_ref, b_ref, act_ref, norm_ref, inv_ref, pre_ref):
    mean, inv = pre_stats(x_ref, w_ref[...], pre_ref)
    inv_ref[...] = inv
    gain, bias = g_ref[...], b_ref[...]

    def fin(i, carry):
        at = pl.ds(pl.multiple_of(i * TILE, TILE), TILE)
        norm = (pre_ref[at, :] - mean) * inv
        norm_ref[at, :] = norm
        act_ref[at, :] = jnp.maximum(norm * gain + bias, 0.0).astype(BF)
        return carry
    lax.fori_loop(0, x_ref.shape[0] // TILE, fin, 0)


def full_spec(shape):
    return pl.BlockSpec(shape, lambda j: (0, 0), pipeline_mode=pl.Buffered(1))


def col_spec(rows):
    return pl.BlockSpec((rows, TILE), lambda j: (0, j))


def row_spec_of(cols):
    return pl.BlockSpec((TILE, cols), lambda j: (j, 0))


def params(limit, **kw):
    return pltpu.CompilerParams(dimension_semantics=('arbitrary',), vmem_limit_bytes=limit << 20, **kw)


def cost(units):
    return pl.CostEstimate(flops=int(units * 2 * 2048 ** 3), bytes_accessed=40 << 20, transcendentals=0)


def layer(x, w, gain, bias):
    rows, width = x.shape[0], w.shape[1]
    return pl.pallas_call(
        layer_kernel, grid=(width // TILE,),
        out_shape=(jax.ShapeDtypeStruct((rows, width), BF), jax.ShapeDtypeStruct((rows, width), F32), jax.ShapeDtypeStruct((1, width), F32)),
        in_specs=[full_spec(x.shape), col_spec(w.shape[0]), col_spec(1), col_spec(1)],
        out_specs=(col_spec(rows), col_spec(rows), col_spec(1)),
        scratch_shapes=[pltpu.VMEM((rows, TILE), F32)],
        compiler_params=params(60), cost_estimate=cost(1), name='layer',
    )(x, w, gain, bias)


def embed_kernel(x_ref, w_ref, emb_ref, norm_ref, inv_ref, other_ref, pre_ref, hold, send_sem, recv_sem):
    j = pl.program_id(0)
    num = pl.num_programs(0)
    me = lax.axis_index(BATCH_AXIS)
    sib = sibling_of(me)

    @pl.when(j == 0)
    def _():
        greet([sib])
    mean, inv = pre_stats(x_ref, w_ref[...], pre_ref)
    inv_ref[...] = inv

    def fin(i, carry):
        at = pl.ds(pl.multiple_of(i * TILE, TILE), TILE)
        norm = (pre_ref[at, :] - mean) * inv
        norm_ref[at, :] = norm
        emb = norm.astype(BF)
        emb_ref[at, :] = emb
        hold[j, at, :] = emb
        return carry
    lax.fori_loop(0, x_ref.shape[0] // TILE, fin, 0)

    def copy(t):
        return remote(hold.at[t], other_ref.at[:, pl.ds(pl.multiple_of(t * TILE, TILE), TILE)], send_sem.at[t], recv_sem.at[t], sib)
    copy(j).start()

    @pl.when(j == num - 1)
    def _():
        def end(t, carry):
            copy(t).wait()
            return carry
        lax.fori_loop(0, num, end, 0)


def embed(x, w):
    rows, width = x.shape[0], w.shape[1]
    tiles = width // TILE
    return pl.pallas_call(
        embed_kernel, grid=(tiles,),
        out_shape=(jax.ShapeDtypeStruct((rows, width), BF), jax.ShapeDtypeStruct((rows, width), F32), jax.ShapeDtypeStruct((1, width), F32), jax.ShapeDtypeStruct((rows, width), BF)),
        in_specs=[full_spec(x.shape), col_spec(w.shape[0])],
        out_specs=(col_spec(rows), col_spec(rows), col_spec(1), pl.BlockSpec(memory_space=pl.ANY)),
        scratch_shapes=[pltpu.VMEM((rows, TILE), F32), pltpu.VMEM((tiles, rows, TILE), BF), pltpu.SemaphoreType.DMA((tiles,)), pltpu.SemaphoreType.DMA((tiles,))],
        compiler_params=params(60, collective_id=1, has_side_effects=True), cost_estimate=cost(1), name='embed',
    )(x, w)


def corr_kernel(lam_ref, emb_ref, other_ref, norm_ref, inv_ref, dout_ref, loss_ref, left, grad_c, scr):
    j = pl.program_id(0)
    rows, width = other_ref.shape
    scale = 1.0 / rows
    lam = lam_ref[0]

    @pl.when(j == 0)
    def _():
        loss_ref[...] = jnp.zeros_like(loss_ref)
    left[...] = emb_ref[...].T

    def corr_step(i, loss):
        at = pl.ds(pl.multiple_of(i * CHUNK, CHUNK), CHUNK)
        corr = mm(left[...], other_ref[:, at]) * scale
        row_id = lax.broadcasted_iota(jnp.int32, corr.shape, 0) + j * TILE
        col_id = lax.broadcasted_iota(jnp.int32, corr.shape, 1) + i * CHUNK
        on_diag = row_id == col_id
        miss = 1.0 - corr
        lam_corr = lam * corr
        grad_c[:, at] = jnp.where(on_diag, -2.0 * miss, 2.0 * lam_corr).astype(BF)
        return loss + fold(jnp.where(on_diag, miss * miss, lam_corr * corr))
    loss = lax.fori_loop(0, width // CHUNK, corr_step, jnp.zeros((8, CHUNK), F32), unroll=True)
    loss_ref[...] += loss

    def emb_step(i, carry):
        at = pl.ds(pl.multiple_of(i * CHUNK, CHUNK), CHUNK)
        val = mm(other_ref[at, :], grad_c[...], 1, 1) * scale
        scr[at, :] = val
        return carry[0] + fold(val), carry[1] + fold(val * norm_ref[at, :])
    zero = jnp.zeros((8, TILE), F32)
    tot, crs = lax.fori_loop(0, rows // CHUNK, emb_step, (zero, zero), unroll=True)
    mean_grad = jnp.sum(tot, axis=0, keepdims=True) / rows
    mean_cross = jnp.sum(crs, axis=0, keepdims=True) / rows
    inv = inv_ref[...]

    def fin(i, carry):
        at = pl.ds(pl.multiple_of(i * TILE, TILE), TILE)
        dout_ref[at, :] = (inv * (scr[at, :] - mean_grad - norm_ref[at, :] * mean_cross)).astype(BF)
        return carry
    lax.fori_loop(0, rows // TILE, fin, 0)


def corr_back(lam_off, emb, other, norm, inv):
    rows, width = emb.shape
    return pl.pallas_call(
        corr_kernel, grid=(width // TILE,),
        out_shape=(jax.ShapeDtypeStruct((rows, width), BF), jax.ShapeDtypeStruct((8, CHUNK), F32)),
        in_specs=[pl.BlockSpec(memory_space=pltpu.SMEM), col_spec(rows), full_spec(other.shape), col_spec(rows), col_spec(1)],
        out_specs=(col_spec(rows), pl.BlockSpec((8, CHUNK), lambda j: (0, 0))),
        scratch_shapes=[pltpu.VMEM((TILE, rows), BF), pltpu.VMEM((TILE, width), BF), pltpu.VMEM((rows, TILE), F32)],
        compiler_params=params(60), cost_estimate=cost(2), name='corr_back',
    )(lam_off.reshape(1), emb, other, norm, inv)


def back_kernel(d_ref, w_ref, norm_ref, inv_ref, g_ref, b_ref, dpre_ref, dg_ref, db_ref, scr):
    rows = d_ref.shape[0]
    gain, bias, inv = g_ref[...], b_ref[...], inv_ref[...]

    def step(i, carry):
        at = pl.ds(pl.multiple_of(i * CHUNK, CHUNK), CHUNK)
        val = mm(d_ref[at, :], w_ref[...], 1, 1)
        norm = norm_ref[at, :]
        val = jnp.where(norm * gain + bias > 0, val, 0.0)
        scr[at, :] = val
        return carry[0] + fold(val), carry[1] + fold(val * norm)
    zero = jnp.zeros((8, TILE), F32)
    tot, crs = lax.fori_loop(0, rows // CHUNK, step, (zero, zero), unroll=True)
    tot = jnp.sum(tot, axis=0, keepdims=True)
    crs = jnp.sum(crs, axis=0, keepdims=True)
    db_ref[...] = tot
    dg_ref[...] = crs
    mean_grad = gain * tot / rows
    mean_cross = gain * crs / rows

    def fin(i, carry):
        at = pl.ds(pl.multiple_of(i * TILE, TILE), TILE)
        dpre_ref[at, :] = (inv * (scr[at, :] * gain - mean_grad - norm_ref[at, :] * mean_cross)).astype(BF)
        return carry
    lax.fori_loop(0, rows // TILE, fin, 0)


def layer_back(grad, w, norm, inv, gain, bias):
    rows, width = norm.shape
    vec = jax.ShapeDtypeStruct((1, width), F32)
    return pl.pallas_call(
        back_kernel, grid=(width // TILE,),
        out_shape=(jax.ShapeDtypeStruct((rows, width), BF), vec, vec),
        in_specs=[full_spec(grad.shape), row_spec_of(w.shape[1]), col_spec(rows), col_spec(1), col_spec(1), col_spec(1)],
        out_specs=(col_spec(rows), col_spec(1), col_spec(1)),
        scratch_shapes=[pltpu.VMEM((rows, TILE), F32)],
        compiler_params=params(60), cost_estimate=cost(1), name='layer_back',
    )(grad, w, norm, inv, gain, bias)


def weights_kernel(acts, grads, small_ref, outs, small_out, lhs, left, rhs, sbuf, rbuf, obuf, small_in, lhs_sem, rhs_sem, ps, pr, os_, or_, ol, ss, sr):
    me = lax.axis_index(BATCH_AXIS)
    core = lax.rem(me, 2)
    sib = sibling_of(me)
    width = outs[0].shape[1]
    half_tiles = outs[0].shape[0] // TILE // 2
    num = len(acts)
    total = num * 2 * half_tiles

    def tile_of(step):
        pos = step % (2 * half_tiles)
        if pos < half_tiles:
            return (1 - core) * half_tiles + pos
        return core * half_tiles + pos - half_tiles

    def cols(tile):
        return pl.ds(pl.multiple_of(tile * TILE, TILE), TILE)

    def load_lhs(step):
        return pltpu.make_async_copy(acts[step // (2 * half_tiles)].at[:, cols(tile_of(step))], lhs.at[step % 2], lhs_sem.at[step % 2])

    def load_rhs(which):
        return pltpu.make_async_copy(grads[which], rhs.at[which % 2], rhs_sem.at[which % 2])

    def part_copy(which, t):
        slot = which * half_tiles + t
        return remote(sbuf.at[t], rbuf.at[slot], ps.at[slot], pr.at[slot], sib)

    def out_rows(which, t):
        return outs[which].at[cols(core * half_tiles + t), :]

    def sum_copy(which, t):
        slot = which * half_tiles + t
        return remote(obuf.at[t % 2], out_rows(which, t), os_.at[slot], or_.at[slot], sib)

    def own_copy(which, t):
        return pltpu.make_async_copy(obuf.at[t % 2], out_rows(which, t), ol.at[which * half_tiles + t])

    load_rhs(0).start()
    load_lhs(0).start()
    greet([sib])
    small_copy = remote(small_ref, small_in, ss, sr, sib)
    small_copy.start()
    for step in range(total):
        which, pos = step // (2 * half_tiles), step % (2 * half_tiles)
        if step + 1 < total:
            load_lhs(step + 1).start()
        if pos == 0:
            load_rhs(which).wait()
            if which + 1 < num:
                load_rhs(which + 1).start()
        load_lhs(step).wait()
        left[...] = lhs[step % 2].T
        t = pos % half_tiles
        if pos < half_tiles:
            if which:
                part_copy(which - 1, t).wait_send()

            def part(i, carry):
                at = pl.ds(pl.multiple_of(i * CHUNK, CHUNK), CHUNK)
                sbuf[t, :, at] = mm(left[...], rhs[which % 2, :, at])
                return carry
            lax.fori_loop(0, width // CHUNK, part, 0)
            part_copy(which, t).start()
        else:
            before = which * half_tiles + t - 2
            if before >= 0:
                sum_copy(before // half_tiles, before % half_tiles).wait_send()
                own_copy(before // half_tiles, before % half_tiles).wait()
            part_copy(which, t).wait_recv()
            slot = which * half_tiles + t

            def whole(i, carry):
                at = pl.ds(pl.multiple_of(i * CHUNK, CHUNK), CHUNK)
                obuf[t % 2, :, at] = mm(left[...], rhs[which % 2, :, at]) + rbuf[slot, :, at]
                return carry
            lax.fori_loop(0, width // CHUNK, whole, 0)
            sum_copy(which, t).start()
            own_copy(which, t).start()
    small_copy.wait()
    small_out[...] = small_ref[...] + small_in[...]
    for t in range(half_tiles):
        part_copy(num - 1, t).wait_send()
        if t >= half_tiles - 2:
            sum_copy(num - 1, t).wait_send()
            own_copy(num - 1, t).wait()
    for which in range(num):
        for t in range(half_tiles):
            sum_copy(which, t).wait_recv()


def weight_grads(acts, grads, small):
    num = len(acts)
    rows = acts[0].shape[0]
    depth, width = acts[0].shape[1], grads[0].shape[1]
    half_tiles = depth // TILE // 2
    slots = num * half_tiles
    anyspec = pl.BlockSpec(memory_space=pl.ANY)
    vmem = pl.BlockSpec(memory_space=pltpu.VMEM)
    dma = pltpu.SemaphoreType.DMA

    def kern(*refs):
        weights_kernel(refs[:num], refs[num:2 * num], refs[2 * num], refs[2 * num + 1:3 * num + 1], *refs[3 * num + 1:])
    return pl.pallas_call(
        kern,
        out_shape=tuple(jax.ShapeDtypeStruct((depth, width), F32) for _ in range(num)) + (jax.ShapeDtypeStruct(small.shape, F32),),
        in_specs=[anyspec] * (2 * num) + [vmem],
        out_specs=tuple([anyspec] * num + [vmem]),
        scratch_shapes=[pltpu.VMEM((2, rows, TILE), BF), pltpu.VMEM((TILE, rows), BF), pltpu.VMEM((2, rows, width), BF),
                        pltpu.VMEM((half_tiles, TILE, width), F32), pltpu.VMEM((slots, TILE, width), F32), pltpu.VMEM((2, TILE, width), F32),
                        pltpu.VMEM(small.shape, F32), dma((2,)), dma((2,)), dma((slots,)), dma((slots,)), dma((slots,)), dma((slots,)), dma((slots,)), dma, dma],
        compiler_params=pltpu.CompilerParams(collective_id=2, has_side_effects=True, vmem_limit_bytes=63 << 20),
        cost_estimate=cost(num), name='weight_grads',
    )(*acts, *grads, small)


def solution(mesh):
    num_devs = mesh.shape[BATCH_AXIS]

    def local_step(feat_a, feat_b, w_one, w_two, w_three, g_one, b_one, g_two, b_two, lam_off):
        first = (lax.axis_index(BATCH_AXIS) % 2) == 0
        feat = gather_rows(jnp.stack([feat_a, feat_b]), num_devs)
        g_one, b_one, g_two, b_two = (v.reshape(1, -1) for v in (g_one, b_one, g_two, b_two))
        act_one, norm_one, inv_one = layer(feat, w_one, g_one, b_one)
        act_two, norm_two, inv_two = layer(act_one, w_two, g_two, b_two)
        emb, norm_out, inv_out, other = embed(act_two, w_three)
        grad_proj, loss = corr_back(lam_off, emb, other, norm_out, inv_out)
        loss_val = jnp.where(first, jnp.sum(loss), 0.0)
        grad_two, dg_two, db_two = layer_back(grad_proj, w_three, norm_two, inv_two, g_two, b_two)
        grad_one, dg_one, db_one = layer_back(grad_two, w_two, norm_one, inv_one, g_one, b_one)
        zero = jnp.zeros_like(dg_one)
        small = jnp.concatenate([dg_one, db_one, dg_two, db_two, zero + loss_val, zero, zero, zero])
        dw_three, dw_two, dw_one, small = weight_grads((act_two, act_one, feat), (grad_proj, grad_two, grad_one), small)
        return (small[4, 0], dw_one, dw_two, dw_three, small[0], small[1], small[2], small[3])

    row_spec = P(BATCH_AXIS, None)
    return jax.shard_map(local_step, mesh=mesh, in_specs=(row_spec, row_spec, P(), P(), P(), P(), P(), P(), P(), P()), out_specs=(P(), P(), P(), P(), P(), P(), P(), P()), check_vma=False)
```

```python
import functools

import jax
import jax.numpy as jnp
from jax import lax
from jax.experimental import pallas as pl
from jax.experimental.pallas import tpu as pltpu
from jax.sharding import PartitionSpec as P

NORM_EPS = 1e-5
BATCH_AXIS = 'data'
MESH_ID = pl.DeviceIdType.MESH
TILE = 256
CHUNK = 512
BF = jnp.bfloat16
F32 = jnp.float32


def mm(lhs, rhs, lhs_dim=1, rhs_dim=0):
    return lax.dot_general(lhs, rhs, (((lhs_dim,), (rhs_dim,)), ((), ())), preferred_element_type=F32)


def fold(val):
    return jnp.sum(val.reshape(val.shape[0] // 8, 8, val.shape[1]), axis=0)


def sibling_of(me):
    return me + 1 - 2 * lax.rem(me, 2)


def greet(peers):
    barrier = pltpu.get_barrier_semaphore()
    for peer in peers:
        pl.semaphore_signal(barrier, inc=1, device_id=(peer,), device_id_type=MESH_ID)
    pl.semaphore_wait(barrier, len(peers))


def remote(src, dst, send_sem, recv_sem, dev):
    return pltpu.make_async_remote_copy(src_ref=src, dst_ref=dst, send_sem=send_sem, recv_sem=recv_sem, device_id=(dev,), device_id_type=MESH_ID)


def gather_kernel(rows, feat_a, feat_b, w_hbm, g_ref, b_ref, out_ref, act_out, pre_out, mean_ref, inv_ref, buf, w_ref, pre, act, tot, sqr,
                  own_sem, sib_s, sib_r, send_sem, recv_sem, w_sem, out_sem, pre_sem, act_sem):
    load_w = pltpu.make_async_copy(w_hbm, w_ref, w_sem)
    load_w.start()
    me = lax.axis_index(BATCH_AXIS)
    core = lax.rem(me, 2)
    sib = sibling_of(me)
    chip = me // 2
    xpos = lax.rem(chip, 2)
    ypos = lax.rem(chip // 2, 2)
    zpos = chip // 4
    x_dev = me + 2 - 4 * xpos
    y_dev = me + 4 - 8 * ypos
    up_dev = jnp.minimum(zpos + 1, 3) * 8 + lax.rem(me, 8)
    down_dev = jnp.maximum(zpos - 1, 0) * 8 + lax.rem(me, 8)
    barrier = pltpu.get_barrier_semaphore()
    for peer in (sib, x_dev, y_dev):
        pl.semaphore_signal(barrier, inc=1, device_id=(peer,), device_id_type=MESH_ID)
    has_up = zpos < 3
    has_down = zpos > 0

    @pl.when(has_up)
    def _():
        pl.semaphore_signal(barrier, inc=1, device_id=(up_dev,), device_id_type=MESH_ID)

    @pl.when(has_down)
    def _():
        pl.semaphore_signal(barrier, inc=1, device_id=(down_dev,), device_id_type=MESH_ID)
    pl.semaphore_wait(barrier, 3 + (1 - (zpos + 1) // 4) + (zpos + 3) // 4)

    def half(idx, part):
        return buf.at[pl.ds(pl.multiple_of(idx * 2 * rows + part * rows, rows), rows), :]

    for which, mine, theirs in ((0, feat_a, feat_b), (1, feat_b, feat_a)):
        @pl.when(core == which)
        def _(mine=mine, theirs=theirs):
            own = pltpu.make_async_copy(mine, half(chip, core), own_sem)
            own.start()
            to_sib = remote(theirs, half(chip, core), sib_s, sib_r, sib)
            to_sib.start()
            own.wait()
            to_sib.wait()

    def piece(idx, part, way, dev):
        return remote(half(idx, part), half(idx, part), send_sem.at[idx * 2 + part, way], recv_sem.at[idx, part], dev)

    def blk(xx, yy, zz):
        return (zz * 2 + yy) * 2 + xx

    def column(zz, part, going_up, going_down):
        idx = blk(xpos, ypos, zz)
        piece(idx, part, 0, x_dev).start()
        piece(idx, part, 1, y_dev).start()
        if going_up:
            @pl.when(has_up)
            def _():
                piece(idx, part, 2, up_dev).start()
        if going_down:
            @pl.when(has_down)
            def _():
                piece(idx, part, 3, down_dev).start()

    def arrived(idx, part):
        piece(idx, part, 0, x_dev).wait_recv()

    def across(zz):
        idx_x = blk(1 - xpos, ypos, zz)
        arrived(idx_x, 0)
        piece(idx_x, 0, 1, y_dev).start()
        idx_y = blk(xpos, 1 - ypos, zz)
        arrived(idx_y, 1)
        piece(idx_y, 1, 0, x_dev).start()

    def plane_rows(zz):
        return pl.ds(pl.multiple_of(zz * 8 * rows, 8 * rows), 8 * rows)

    def feat_copy(zz):
        return pltpu.make_async_copy(buf.at[plane_rows(zz), :], out_ref.at[plane_rows(zz), :], out_sem.at[zz])

    def pre_copy(zz):
        return pltpu.make_async_copy(pre.at[plane_rows(zz), :], pre_out.at[plane_rows(zz), :], pre_sem.at[zz])

    def multiply(zz):
        arrived(blk(1 - xpos, ypos, zz), 1)
        arrived(blk(xpos, 1 - ypos, zz), 0)
        arrived(blk(1 - xpos, 1 - ypos, zz), 0)
        arrived(blk(1 - xpos, 1 - ypos, zz), 1)
        feat_copy(zz).start()

        def step(i, carry):
            at = pl.ds(pl.multiple_of(i * CHUNK, CHUNK), CHUNK)
            val = mm(buf[plane_rows(zz), :], w_ref[:, at])
            pre[plane_rows(zz), at] = val
            tot[:, at] += fold(val)
            sqr[:, at] += fold(val * val)
            return carry
        lax.fori_loop(0, pre.shape[1] // CHUNK, step, 0)
        pre_copy(zz).start()

    for part in range(2):
        column(zpos, part, True, True)
    tot[...] = jnp.zeros_like(tot)
    sqr[...] = jnp.zeros_like(sqr)
    load_w.wait()

    def level(dist, carry):
        for sign in (-1, 1):
            zz = zpos + sign * dist

            @pl.when(jnp.logical_and(zz >= 0, zz < 4))
            def _(zz=zz, sign=sign):
                for part in range(2):
                    arrived(blk(xpos, ypos, zz), part)
                    column(zz, part, sign < 0, sign > 0)
            near = zpos + sign * (dist - 1)

            @pl.when(jnp.logical_and(jnp.logical_and(near >= 0, near < 4), dist > (1 if sign > 0 else 0)))
            def _(near=near):
                across(near)
            done = zpos + sign * (dist - 2)

            @pl.when(jnp.logical_and(jnp.logical_and(done >= 0, done < 4), dist > (2 if sign > 0 else 1)))
            def _(done=done):
                multiply(done)
        return carry
    lax.fori_loop(1, 6, level, 0)
    count = buf.shape[0]
    mean = jnp.sum(tot[...], axis=0, keepdims=True) / count
    inv = lax.rsqrt(jnp.sum(sqr[...], axis=0, keepdims=True) / count - mean * mean + NORM_EPS)
    mean_ref[...] = mean
    inv_ref[...] = inv

    def act_copy(i):
        at = pl.ds(pl.multiple_of(i * TILE, TILE), TILE)
        return pltpu.make_async_copy(act.at[at, :], act_out.at[at, :], act_sem.at[i])

    def fin(i, carry):
        def part(k, carry):
            at = pl.ds(pl.multiple_of(i * TILE + k * 32, 32), 32)
            norm = (pre[at, :] - mean_ref[...]) * inv_ref[...]
            act[at, :] = jnp.maximum(norm * g_ref[...] + b_ref[...], 0.0).astype(BF)
            return carry
        lax.fori_loop(0, TILE // 32, part, 0)
        act_copy(i).start()
        return carry
    lax.fori_loop(0, count // TILE, fin, 0)

    def drain(zz, carry):
        col = blk(xpos, ypos, zz)
        for part in range(2):
            piece(col, part, 0, x_dev).wait_send()
            piece(col, part, 1, y_dev).wait_send()

            @pl.when(jnp.logical_and(has_up, zz <= zpos))
            def _(part=part):
                piece(col, part, 2, up_dev).wait_send()

            @pl.when(jnp.logical_and(has_down, zz >= zpos))
            def _(part=part):
                piece(col, part, 3, down_dev).wait_send()
        piece(blk(1 - xpos, ypos, zz), 0, 1, y_dev).wait_send()
        piece(blk(xpos, 1 - ypos, zz), 1, 0, x_dev).wait_send()
        feat_copy(zz).wait()
        pre_copy(zz).wait()
        return carry
    lax.fori_loop(0, 4, drain, 0)

    def act_wait(i, carry):
        act_copy(i).wait()
        return carry
    lax.fori_loop(0, count // TILE, act_wait, 0)


def gather_layer(feat_a, feat_b, w, gain, bias, num_devs):
    rows, depth = feat_a.shape
    count, width = num_devs * rows, w.shape[1]
    chips = num_devs // 2
    dma = pltpu.SemaphoreType.DMA
    hbm, vmem = pl.BlockSpec(memory_space=pl.ANY), pl.BlockSpec(memory_space=pltpu.VMEM)
    vec = jax.ShapeDtypeStruct((1, width), F32)
    return pl.pallas_call(
        functools.partial(gather_kernel, rows),
        out_shape=(jax.ShapeDtypeStruct((count, depth), BF), jax.ShapeDtypeStruct((count, width), BF), jax.ShapeDtypeStruct((count, width), F32), vec, vec),
        in_specs=[vmem, vmem, hbm, vmem, vmem],
        out_specs=(hbm, hbm, hbm, vmem, vmem),
        scratch_shapes=[pltpu.VMEM((count, depth), BF), pltpu.VMEM(w.shape, BF), pltpu.VMEM((count, width), F32), pltpu.VMEM((count, width), BF),
                        pltpu.VMEM((8, width), F32), pltpu.VMEM((8, width), F32), dma, dma, dma,
                        dma((2 * chips, 4)), dma((chips, 2)), dma, dma((4,)), dma((4,)), dma((count // TILE,))],
        compiler_params=pltpu.CompilerParams(collective_id=0, has_side_effects=True, vmem_limit_bytes=60 << 20),
        name='gather_layer',
    )(feat_a, feat_b, w, gain, bias)


def at_chunk(i):
    return pl.ds(pl.multiple_of(i * CHUNK, CHUNK), CHUNK)


def at_tile(i):
    return pl.ds(pl.multiple_of(i * TILE, TILE), TILE)


def any_spec():
    return pl.BlockSpec(memory_space=pl.ANY)


def now(j, tiles):
    return jnp.minimum(j, tiles - 1)


def past(j):
    return jnp.maximum(j - 1, 0)


def col_now(rows, tiles):
    return pl.BlockSpec((rows, TILE), lambda j: (0, now(j, tiles)))


def col_past(rows):
    return pl.BlockSpec((rows, TILE), lambda j: (0, past(j)))


def row_now(cols, tiles):
    return pl.BlockSpec((TILE, cols), lambda j: (now(j, tiles), 0))


def row_past(cols):
    return pl.BlockSpec((TILE, cols), lambda j: (past(j), 0))


def row_same(cols):
    return pl.BlockSpec((TILE, cols), lambda j: (j, 0))


def col_same(rows):
    return pl.BlockSpec((rows, TILE), lambda j: (0, j))


def params(**kw):
    return pltpu.CompilerParams(dimension_semantics=('arbitrary',), vmem_limit_bytes=60 << 20, **kw)


def cost(units):
    return pl.CostEstimate(flops=int(units * 2 * 2048 ** 3), bytes_accessed=40 << 20, transcendentals=0)


def row_load(src, dst, sem, i):
    return pltpu.make_async_copy(src.at[at_chunk(i), :], dst.at[at_chunk(i), :], sem.at[i])


def col_load(src, dst, sem, i):
    return pltpu.make_async_copy(src.at[:, at_chunk(i)], dst.at[:, at_chunk(i)], sem.at[i])


def schedule(tiles, chunks, load, begin, mul, fin, end):
    j = pl.program_id(0)
    zero = (jnp.zeros((8, TILE), F32),) * 2

    @pl.when(j == 0)
    def _():
        for i in range(chunks):
            load(i).start()
        begin()

        def step(i, sums):
            load(i).wait()
            return mul(i, sums)
        end(lax.fori_loop(0, chunks, step, zero))

    @pl.when(jnp.logical_and(j > 0, j < tiles))
    def _():
        begin()
        sums = zero
        for i in range(chunks):
            fin(i)
            sums = mul(i, sums)
        end(sums)

    @pl.when(j == tiles)
    def _():
        def step(i, carry):
            fin(i)
            return carry
        lax.fori_loop(0, chunks, step, 0)


def row_sum(val):
    return jnp.sum(val, axis=0, keepdims=True)


def layer_kernel(tiles, x_hbm, w_ref, g_ref, b_ref, act_ref, norm_ref, inv_ref, x_ref, x_sem, pre, mean_s, inv_s):
    rows = x_ref.shape[0]

    def mul(i, sums):
        val = mm(x_ref[at_chunk(i), :], w_ref[...])
        pre[at_chunk(i), :] = val
        return sums[0] + fold(val), sums[1] + fold(val * val)

    def fin(i):
        norm = (pre[at_chunk(i), :] - mean_s[...]) * inv_s[...]
        norm_ref[at_chunk(i), :] = norm
        act_ref[at_chunk(i), :] = jnp.maximum(norm * g_ref[...] + b_ref[...], 0.0).astype(BF)

    def end(sums):
        mean = row_sum(sums[0]) / rows
        mean_s[...] = mean
        inv_s[...] = lax.rsqrt(row_sum(sums[1]) / rows - mean * mean + NORM_EPS)

    @pl.when(pl.program_id(0) > 0)
    def _():
        inv_ref[...] = inv_s[...]
    schedule(tiles, rows // CHUNK, functools.partial(row_load, x_hbm, x_ref, x_sem), lambda: None, mul, fin, end)


def layer(x, w, gain, bias):
    rows, width = x.shape[0], w.shape[1]
    tiles = width // TILE
    return pl.pallas_call(
        functools.partial(layer_kernel, tiles), grid=(tiles + 1,),
        out_shape=(jax.ShapeDtypeStruct((rows, width), BF), jax.ShapeDtypeStruct((rows, width), F32), jax.ShapeDtypeStruct((1, width), F32)),
        in_specs=[any_spec(), col_now(w.shape[0], tiles), col_past(1), col_past(1)],
        out_specs=(col_past(rows), col_past(rows), col_past(1)),
        scratch_shapes=[pltpu.VMEM(x.shape, BF), pltpu.SemaphoreType.DMA((rows // CHUNK,)), pltpu.VMEM((rows, TILE), F32), pltpu.VMEM((1, TILE), F32), pltpu.VMEM((1, TILE), F32)],
        compiler_params=params(), cost_estimate=cost(1), name='layer',
    )(x, w, gain, bias)


def share(hold, other_ref, send_sem, recv_sem, t):
    return remote(hold.at[t], other_ref.at[:, at_tile(t)], send_sem.at[t], recv_sem.at[t], sibling_of(lax.axis_index(BATCH_AXIS)))


def share_tiles(j, tiles, copy):
    @pl.when(j > 0)
    def _():
        copy(j - 1).start()

    @pl.when(j == tiles)
    def _():
        def last(t, carry):
            copy(t).wait()
            return carry
        lax.fori_loop(0, tiles, last, 0)


def embed_kernel(tiles, x_hbm, w_ref, emb_ref, norm_ref, inv_ref, other_ref, x_ref, x_sem, pre, mean_s, inv_s, hold, send_sem, recv_sem):
    rows = x_ref.shape[0]
    j = pl.program_id(0)

    @pl.when(j == 0)
    def _():
        greet([sibling_of(lax.axis_index(BATCH_AXIS))])

    def mul(i, sums):
        val = mm(x_ref[at_chunk(i), :], w_ref[...])
        pre[at_chunk(i), :] = val
        return sums[0] + fold(val), sums[1] + fold(val * val)

    def fin(i):
        norm = (pre[at_chunk(i), :] - mean_s[...]) * inv_s[...]
        norm_ref[at_chunk(i), :] = norm
        emb = norm.astype(BF)
        emb_ref[at_chunk(i), :] = emb
        hold[past(j), at_chunk(i), :] = emb

    def end(sums):
        mean = row_sum(sums[0]) / rows
        mean_s[...] = mean
        inv_s[...] = lax.rsqrt(row_sum(sums[1]) / rows - mean * mean + NORM_EPS)

    @pl.when(j > 0)
    def _():
        inv_ref[...] = inv_s[...]
    schedule(tiles, rows // CHUNK, functools.partial(row_load, x_hbm, x_ref, x_sem), lambda: None, mul, fin, end)
    share_tiles(j, tiles, functools.partial(share, hold, other_ref, send_sem, recv_sem))


def share_scratch(rows, tiles):
    return [pltpu.VMEM((tiles, rows, TILE), BF), pltpu.SemaphoreType.DMA((tiles,)), pltpu.SemaphoreType.DMA((tiles,))]


def embed(x, w):
    rows, width = x.shape[0], w.shape[1]
    tiles = width // TILE
    return pl.pallas_call(
        functools.partial(embed_kernel, tiles), grid=(tiles + 1,),
        out_shape=(jax.ShapeDtypeStruct((rows, width), BF), jax.ShapeDtypeStruct((rows, width), F32), jax.ShapeDtypeStruct((1, width), F32), jax.ShapeDtypeStruct((rows, width), BF)),
        in_specs=[any_spec(), col_now(w.shape[0], tiles)],
        out_specs=(col_past(rows), col_past(rows), col_past(1), any_spec()),
        scratch_shapes=[pltpu.VMEM(x.shape, BF), pltpu.SemaphoreType.DMA((rows // CHUNK,)), pltpu.VMEM((rows, TILE), F32), pltpu.VMEM((1, TILE), F32), pltpu.VMEM((1, TILE), F32)] + share_scratch(rows, tiles),
        compiler_params=params(collective_id=1, has_side_effects=True), cost_estimate=cost(1), name='embed',
    )(x, w)


def corr_kernel(lam_ref, emb_ref, other_ref, norm_ref, inv_ref, dout_ref, loss_ref, left, grad_c, scr):
    j = pl.program_id(0)
    rows, width = other_ref.shape
    scale = 1.0 / rows
    lam = lam_ref[0]

    @pl.when(j == 0)
    def _():
        loss_ref[...] = jnp.zeros_like(loss_ref)
    left[...] = emb_ref[...].T

    def corr_step(i, loss):
        at = pl.ds(pl.multiple_of(i * CHUNK, CHUNK), CHUNK)
        corr = mm(left[...], other_ref[:, at]) * scale
        row_id = lax.broadcasted_iota(jnp.int32, corr.shape, 0) + j * TILE
        col_id = lax.broadcasted_iota(jnp.int32, corr.shape, 1) + i * CHUNK
        on_diag = row_id == col_id
        miss = 1.0 - corr
        lam_corr = lam * corr
        grad_c[:, at] = jnp.where(on_diag, -2.0 * miss, 2.0 * lam_corr).astype(BF)
        return loss + fold(jnp.where(on_diag, miss * miss, lam_corr * corr))
    loss = lax.fori_loop(0, width // CHUNK, corr_step, jnp.zeros((8, CHUNK), F32), unroll=True)
    loss_ref[...] += loss

    def emb_step(i, carry):
        at = pl.ds(pl.multiple_of(i * CHUNK, CHUNK), CHUNK)
        val = mm(other_ref[at, :], grad_c[...], 1, 1) * scale
        scr[at, :] = val
        return carry[0] + fold(val), carry[1] + fold(val * norm_ref[at, :])
    zero = jnp.zeros((8, TILE), F32)
    tot, crs = lax.fori_loop(0, rows // CHUNK, emb_step, (zero, zero), unroll=True)
    mean_grad = jnp.sum(tot, axis=0, keepdims=True) / rows
    mean_cross = jnp.sum(crs, axis=0, keepdims=True) / rows
    inv = inv_ref[...]

    def fin(i, carry):
        at = pl.ds(pl.multiple_of(i * TILE, TILE), TILE)
        dout_ref[at, :] = (inv * (scr[at, :] - mean_grad - norm_ref[at, :] * mean_cross)).astype(BF)
        return carry
    lax.fori_loop(0, rows // TILE, fin, 0)


def corr_back(lam_off, emb, other, norm, inv):
    rows, width = emb.shape
    return pl.pallas_call(
        corr_kernel, grid=(width // TILE,),
        out_shape=(jax.ShapeDtypeStruct((rows, width), BF), jax.ShapeDtypeStruct((8, CHUNK), F32)),
        in_specs=[pl.BlockSpec(memory_space=pltpu.SMEM), col_same(rows), pl.BlockSpec(other.shape, lambda j: (0, 0), pipeline_mode=pl.Buffered(1)), col_same(rows), col_same(1)],
        out_specs=(col_same(rows), pl.BlockSpec((8, CHUNK), lambda j: (0, 0))),
        scratch_shapes=[pltpu.VMEM((TILE, rows), BF), pltpu.VMEM((TILE, width), BF), pltpu.VMEM((rows, TILE), F32)],
        compiler_params=params(), cost_estimate=cost(2), name='corr_back',
    )(lam_off.reshape(1), emb, other, norm, inv)


def back_kernel(tiles, layered, act_hbm, d_hbm, *refs):
    if layered:
        w_ref, pre_ref, mean_ref, scale_ref, inv_ref, g_ref, b_ref, g_old, dpre_ref, dg_ref, db_ref, dw_out = refs[:12]
        d_ref, d_sem, lhs, lhs_sem, sbuf, rbuf, ps, pr, os_, or_, ol, scr, norm_s, grad_s, cross_s = refs[12:]
    else:
        small_ref, dw_out, small_out = refs[:3]
        d_ref, d_sem, lhs, lhs_sem, sbuf, rbuf, ps, pr, os_, or_, ol, small_in, ss, sr = refs[3:]
    step = pl.program_id(0)
    rows, width = d_ref.shape
    half = sbuf.shape[0]
    chunks = width // CHUNK
    me = lax.axis_index(BATCH_AXIS)
    core = lax.rem(me, 2)
    sib = sibling_of(me)
    after = step - half
    if layered:
        turn, place = after // 3, lax.rem(after, 3)
        own_turn = jnp.logical_and(jnp.logical_and(after >= 0, after < 3 * half), place == 1)
        tile_turn = jnp.logical_and(jnp.logical_and(after >= 0, after < 3 * half), place != 1)
        last_step = 3 * half
    else:
        turn = after
        own_turn = after >= 0
        last_step = half - 1

    def load_left(q):
        mine = q // half
        tile = (mine * core + (1 - mine) * (1 - core)) * half + q - mine * half
        return pltpu.make_async_copy(act_hbm.at[:, at_tile(tile)], lhs.at[lax.rem(q, 2)], lhs_sem.at[lax.rem(q, 2)])

    def part_copy(t):
        return remote(sbuf.at[t], rbuf.at[t], ps.at[t], pr.at[t], sib)

    def result_rows(t):
        return dw_out.at[at_tile(core * half + t), :]

    def sum_copy(t):
        return remote(sbuf.at[t], result_rows(t), os_.at[t], or_.at[t], sib)

    def own_copy(t):
        return pltpu.make_async_copy(sbuf.at[t], result_rows(t), ol.at[t])

    def load_d(i):
        return col_load(d_hbm, d_ref, d_sem, i)

    def product(q, i):
        return mm(lhs[lax.rem(q, 2)], d_ref[:, at_chunk(i)], 0, 0)

    @pl.when(step == 0)
    def _():
        load_left(0).start()
        for i in range(chunks):
            load_d(i).start()
        load_left(1).start()
        greet([sib])
        if not layered:
            remote(small_ref, small_in, ss, sr, sib).start()
        load_left(0).wait()

        def first(i, carry):
            load_d(i).wait()
            sbuf[0, :, at_chunk(i)] = product(0, i)
            return carry
        lax.fori_loop(0, chunks, first, 0)
        part_copy(0).start()

    @pl.when(jnp.logical_and(step > 0, step < half))
    def _():
        load_left(step + 1).start()
        load_left(step).wait()
        for i in range(chunks):
            sbuf[step, :, at_chunk(i)] = product(step, i)
        part_copy(step).start()

    if layered:
        def mul(i, sums):
            val = mm(d_ref[at_chunk(i), :], w_ref[...], 1, 1)
            norm = (pre_ref[at_chunk(i), :] - mean_ref[...]) * scale_ref[...]
            val = jnp.where(norm * g_ref[...] + b_ref[...] > 0, val, 0.0)
            scr[at_chunk(i), :] = val
            norm_s[at_chunk(i), :] = norm
            return sums[0] + fold(val), sums[1] + fold(val * norm)

        def fin(i):
            dpre_ref[at_chunk(i), :] = (inv_ref[...] * (scr[at_chunk(i), :] * g_old[...] - grad_s[...] - norm_s[at_chunk(i), :] * cross_s[...])).astype(BF)
        zero = (jnp.zeros((8, TILE), F32),) * 2

        @pl.when(tile_turn)
        def _():
            sums = zero
            for i in range(rows // CHUNK):
                fin(i)
                sums = mul(i, sums)
            tot, crs = row_sum(sums[0]), row_sum(sums[1])
            db_ref[...] = tot
            dg_ref[...] = crs
            grad_s[...] = g_ref[...] * tot / rows
            cross_s[...] = g_ref[...] * crs / rows

        @pl.when(after == last_step)
        def _():
            def last(i, carry):
                fin(i)
                return carry
            lax.fori_loop(0, rows // CHUNK, last, 0)

    @pl.when(own_turn)
    def _():
        t = turn
        q = t + half

        @pl.when(t + 1 < half)
        def _():
            load_left(q + 1).start()
        load_left(q).wait()
        part_copy(t).wait()
        for i in range(chunks):
            sbuf[t, :, at_chunk(i)] = product(q, i) + rbuf[t, :, at_chunk(i)]
        sum_copy(t).start()
        own_copy(t).start()

    @pl.when(after == last_step)
    def _():
        def end(k, carry):
            sum_copy(k).wait()
            own_copy(k).wait()
            return carry
        lax.fori_loop(0, half, end, 0)
        if not layered:
            remote(small_ref, small_in, ss, sr, sib).wait()
            small_out[...] = small_ref[...] + small_in[...]


def layer_back(ident, act, grad, layer_args=None, small=None):
    rows, width = grad.shape
    depth = act.shape[1]
    half = depth // TILE // 2
    dma = pltpu.SemaphoreType.DMA
    hbm = any_spec()
    scratch = [pltpu.VMEM(grad.shape, BF), dma((width // CHUNK,)), pltpu.VMEM((2, rows, TILE), BF), dma((2,)), pltpu.VMEM((half, TILE, width), F32),
               pltpu.VMEM((half, TILE, width), F32)] + [dma((half,))] * 5
    dw = jax.ShapeDtypeStruct((depth, width), F32)
    if layer_args is not None:
        w, pre, mean, scale, inv, gain, bias = layer_args
        tiles = w.shape[0] // TILE

        def cur(s):
            return jnp.clip((2 * jnp.maximum(s - half, 0) + 1) // 3, 0, tiles - 1)

        def old(s):
            return jnp.clip((2 * jnp.maximum(s - half, 0) + 1) // 3 - 1, 0, tiles - 1)
        vec_cur = pl.BlockSpec((1, TILE), lambda s: (0, cur(s)))
        vec_old = pl.BlockSpec((1, TILE), lambda s: (0, old(s)))
        in_specs = [hbm, hbm, pl.BlockSpec((TILE, w.shape[1]), lambda s: (cur(s), 0)), pl.BlockSpec((rows, TILE), lambda s: (0, cur(s))),
                    vec_cur, vec_cur, vec_old, vec_cur, vec_cur, vec_old]
        out_specs = (pl.BlockSpec((rows, TILE), lambda s: (0, old(s))), vec_cur, vec_cur, hbm)
        vec = jax.ShapeDtypeStruct((1, depth), F32)
        out_shape = (jax.ShapeDtypeStruct((rows, depth), BF), vec, vec, dw)
        scratch += [pltpu.VMEM((rows, TILE), F32), pltpu.VMEM((rows, TILE), F32), pltpu.VMEM((1, TILE), F32), pltpu.VMEM((1, TILE), F32)]
        args = (act, grad, w, pre, mean, scale, inv, gain, bias, gain)
        steps = 2 * half + tiles + 1
    else:
        tiles = 0
        one = pl.BlockSpec(small.shape, lambda s: (0, 0))
        in_specs = [hbm, hbm, one]
        out_specs = (hbm, one)
        out_shape = (dw, jax.ShapeDtypeStruct(small.shape, F32))
        scratch += [pltpu.VMEM(small.shape, F32), dma, dma]
        args = (act, grad, small)
        steps = 2 * half
    return pl.pallas_call(
        functools.partial(back_kernel, tiles, layer_args is not None), grid=(steps,),
        out_shape=out_shape, in_specs=in_specs, out_specs=out_specs, scratch_shapes=scratch,
        compiler_params=params(collective_id=ident, has_side_effects=True), cost_estimate=cost(2), name='back_%d' % ident,
    )(*args)


def solution(mesh):
    num_devs = mesh.shape[BATCH_AXIS]

    def local_step(feat_a, feat_b, w_one, w_two, w_three, g_one, b_one, g_two, b_two, lam_off):
        first = lax.rem(lax.axis_index(BATCH_AXIS), 2) == 0
        g_one, b_one, g_two, b_two = (v.reshape(1, -1) for v in (g_one, b_one, g_two, b_two))
        feat, act_one, pre_one, mean_one, inv_one = gather_layer(feat_a, feat_b, w_one, g_one, b_one, num_devs)
        act_two, norm_two, inv_two = layer(act_one, w_two, g_two, b_two)
        emb, norm_out, inv_out, other = embed(act_two, w_three)
        grad_out, loss = corr_back(lam_off, emb, other, norm_out, inv_out)
        loss_val = jnp.where(first, jnp.sum(loss), 0.0)
        zero, one = jnp.zeros_like(g_two), jnp.ones_like(g_two)
        grad_two, dg_two, db_two, dw_three = layer_back(2, act_two, grad_out, (w_three, norm_two, zero, one, inv_two, g_two, b_two))
        grad_one, dg_one, db_one, dw_two = layer_back(3, act_one, grad_two, (w_two, pre_one, mean_one, inv_one, inv_one, g_one, b_one))
        small = jnp.concatenate([dg_one, db_one, dg_two, db_two, zero + loss_val, zero, zero, zero])
        dw_one, small = layer_back(4, feat, grad_one, small=small)
        return (small[4, 0], dw_one, dw_two, dw_three, small[0], small[1], small[2], small[3])

    row_spec = P(BATCH_AXIS, None)
    return jax.shard_map(local_step, mesh=mesh, in_specs=(row_spec, row_spec, P(), P(), P(), P(), P(), P(), P(), P()), out_specs=(P(), P(), P(), P(), P(), P(), P(), P()), check_vma=False)
```

```python
import functools

import jax
import jax.numpy as jnp
from jax import lax
from jax.experimental import pallas as pl
from jax.experimental.pallas import tpu as pltpu
from jax.sharding import PartitionSpec as P

NORM_EPS = 1e-5
BATCH_AXIS = 'data'
MESH_ID = pl.DeviceIdType.MESH
TILE = 256
CHUNK = 512
BF = jnp.bfloat16
F32 = jnp.float32


def mm(lhs, rhs, lhs_dim=1, rhs_dim=0):
    return lax.dot_general(lhs, rhs, (((lhs_dim,), (rhs_dim,)), ((), ())), preferred_element_type=F32)


def fold(val):
    return jnp.sum(val.reshape(val.shape[0] // 8, 8, val.shape[1]), axis=0)


def sibling_of(me):
    return me + 1 - 2 * lax.rem(me, 2)


def greet(peers):
    barrier = pltpu.get_barrier_semaphore()
    for peer in peers:
        pl.semaphore_signal(barrier, inc=1, device_id=(peer,), device_id_type=MESH_ID)
    pl.semaphore_wait(barrier, len(peers))


def remote(src, dst, send_sem, recv_sem, dev):
    return pltpu.make_async_remote_copy(src_ref=src, dst_ref=dst, send_sem=send_sem, recv_sem=recv_sem, device_id=(dev,), device_id_type=MESH_ID)


def gather_kernel(rows, feat_a, feat_b, w_hbm, g_ref, b_ref, out_ref, act_out, pre_out, mean_ref, inv_ref, buf, w_ref, pre, act, tot, sqr,
                  own_sem, sib_s, sib_r, send_sem, recv_sem, w_sem, out_sem, pre_sem, act_sem):
    load_w = pltpu.make_async_copy(w_hbm, w_ref, w_sem)
    load_w.start()
    me = lax.axis_index(BATCH_AXIS)
    core = lax.rem(me, 2)
    sib = sibling_of(me)
    chip = me // 2
    xpos = lax.rem(chip, 2)
    ypos = lax.rem(chip // 2, 2)
    zpos = chip // 4
    x_dev = me + 2 - 4 * xpos
    y_dev = me + 4 - 8 * ypos
    up_dev = jnp.minimum(zpos + 1, 3) * 8 + lax.rem(me, 8)
    down_dev = jnp.maximum(zpos - 1, 0) * 8 + lax.rem(me, 8)
    barrier = pltpu.get_barrier_semaphore()
    for peer in (sib, x_dev, y_dev):
        pl.semaphore_signal(barrier, inc=1, device_id=(peer,), device_id_type=MESH_ID)
    has_up = zpos < 3
    has_down = zpos > 0

    @pl.when(has_up)
    def _():
        pl.semaphore_signal(barrier, inc=1, device_id=(up_dev,), device_id_type=MESH_ID)

    @pl.when(has_down)
    def _():
        pl.semaphore_signal(barrier, inc=1, device_id=(down_dev,), device_id_type=MESH_ID)
    pl.semaphore_wait(barrier, 3 + (1 - (zpos + 1) // 4) + (zpos + 3) // 4)

    def half(idx, part):
        return buf.at[pl.ds(pl.multiple_of(idx * 2 * rows + part * rows, rows), rows), :]

    for which, mine, theirs in ((0, feat_a, feat_b), (1, feat_b, feat_a)):
        @pl.when(core == which)
        def _(mine=mine, theirs=theirs):
            own = pltpu.make_async_copy(mine, half(chip, core), own_sem)
            own.start()
            remote(theirs, half(chip, core), sib_s, sib_r, sib).start()
            own.wait()

    def piece(idx, part, way, dev):
        return remote(half(idx, part), half(idx, part), send_sem.at[idx * 2 + part, way], recv_sem.at[idx, part], dev)

    def blk(xx, yy, zz):
        return (zz * 2 + yy) * 2 + xx

    def column(zz, part, going_up, going_down):
        idx = blk(xpos, ypos, zz)
        piece(idx, part, 0, x_dev).start()
        piece(idx, part, 1, y_dev).start()
        if going_up:
            @pl.when(has_up)
            def _():
                piece(idx, part, 2, up_dev).start()
        if going_down:
            @pl.when(has_down)
            def _():
                piece(idx, part, 3, down_dev).start()

    def arrived(idx, part):
        piece(idx, part, 0, x_dev).wait_recv()

    def across(zz):
        idx_x = blk(1 - xpos, ypos, zz)
        arrived(idx_x, 0)
        piece(idx_x, 0, 1, y_dev).start()
        idx_y = blk(xpos, 1 - ypos, zz)
        arrived(idx_y, 1)
        piece(idx_y, 1, 0, x_dev).start()

    def plane_rows(zz):
        return pl.ds(pl.multiple_of(zz * 8 * rows, 8 * rows), 8 * rows)

    def feat_copy(zz):
        return pltpu.make_async_copy(buf.at[plane_rows(zz), :], out_ref.at[plane_rows(zz), :], out_sem.at[zz])

    def pre_copy(zz):
        return pltpu.make_async_copy(pre.at[plane_rows(zz), :], pre_out.at[plane_rows(zz), :], pre_sem.at[zz])

    def multiply(zz):
        for near_y in (True, False):
            yy = ypos if near_y else 1 - ypos
            if near_y:
                arrived(blk(1 - xpos, ypos, zz), 1)
            else:
                arrived(blk(xpos, 1 - ypos, zz), 0)
                arrived(blk(1 - xpos, 1 - ypos, zz), 0)
                arrived(blk(1 - xpos, 1 - ypos, zz), 1)
            here = pl.ds(pl.multiple_of((zz * 2 + yy) * 4 * rows, 4 * rows), 4 * rows)

            def step(i, carry):
                at = pl.ds(pl.multiple_of(i * CHUNK, CHUNK), CHUNK)
                val = mm(buf[here, :], w_ref[:, at])
                pre[here, at] = val
                tot[:, at] += fold(val)
                sqr[:, at] += fold(val * val)
                return carry
            lax.fori_loop(0, pre.shape[1] // CHUNK, step, 0)
        feat_copy(zz).start()
        pre_copy(zz).start()

    column(zpos, core, True, True)
    tot[...] = jnp.zeros_like(tot)
    sqr[...] = jnp.zeros_like(sqr)
    remote(feat_a, half(chip, core), sib_s, sib_r, sib).wait()
    column(zpos, 1 - core, True, True)
    load_w.wait()

    def level(dist, carry):
        for sign in (-1, 1):
            zz = zpos + sign * dist

            @pl.when(jnp.logical_and(zz >= 0, zz < 4))
            def _(zz=zz, sign=sign):
                for part in range(2):
                    arrived(blk(xpos, ypos, zz), part)
                    column(zz, part, sign < 0, sign > 0)
            near = zpos + sign * (dist - 1)

            @pl.when(jnp.logical_and(jnp.logical_and(near >= 0, near < 4), dist > (1 if sign > 0 else 0)))
            def _(near=near):
                across(near)
            done = zpos + sign * (dist - 2)

            @pl.when(jnp.logical_and(jnp.logical_and(done >= 0, done < 4), dist > (2 if sign > 0 else 1)))
            def _(done=done):
                multiply(done)
        return carry
    lax.fori_loop(1, 6, level, 0)
    count = buf.shape[0]
    mean = jnp.sum(tot[...], axis=0, keepdims=True) / count
    inv = lax.rsqrt(jnp.sum(sqr[...], axis=0, keepdims=True) / count - mean * mean + NORM_EPS)
    mean_ref[...] = mean
    inv_ref[...] = inv

    def act_copy(i):
        at = pl.ds(pl.multiple_of(i * TILE, TILE), TILE)
        return pltpu.make_async_copy(act.at[at, :], act_out.at[at, :], act_sem.at[i])

    def fin(i, carry):
        def part(k, carry):
            at = pl.ds(pl.multiple_of(i * TILE + k * 32, 32), 32)
            norm = (pre[at, :] - mean_ref[...]) * inv_ref[...]
            act[at, :] = jnp.maximum(norm * g_ref[...] + b_ref[...], 0.0).astype(BF)
            return carry
        lax.fori_loop(0, TILE // 32, part, 0)
        act_copy(i).start()
        return carry
    lax.fori_loop(0, count // TILE, fin, 0)

    def drain(zz, carry):
        col = blk(xpos, ypos, zz)
        for part in range(2):
            piece(col, part, 0, x_dev).wait_send()
            piece(col, part, 1, y_dev).wait_send()

            @pl.when(jnp.logical_and(has_up, zz <= zpos))
            def _(part=part):
                piece(col, part, 2, up_dev).wait_send()

            @pl.when(jnp.logical_and(has_down, zz >= zpos))
            def _(part=part):
                piece(col, part, 3, down_dev).wait_send()
        piece(blk(1 - xpos, ypos, zz), 0, 1, y_dev).wait_send()
        piece(blk(xpos, 1 - ypos, zz), 1, 0, x_dev).wait_send()
        feat_copy(zz).wait()
        pre_copy(zz).wait()
        return carry
    lax.fori_loop(0, 4, drain, 0)

    def act_wait(i, carry):
        act_copy(i).wait()
        return carry
    lax.fori_loop(0, count // TILE, act_wait, 0)


def gather_layer(feat_a, feat_b, w, gain, bias, num_devs):
    rows, depth = feat_a.shape
    count, width = num_devs * rows, w.shape[1]
    chips = num_devs // 2
    dma = pltpu.SemaphoreType.DMA
    hbm, vmem = pl.BlockSpec(memory_space=pl.ANY), pl.BlockSpec(memory_space=pltpu.VMEM)
    vec = jax.ShapeDtypeStruct((1, width), F32)
    return pl.pallas_call(
        functools.partial(gather_kernel, rows),
        out_shape=(jax.ShapeDtypeStruct((count, depth), BF), jax.ShapeDtypeStruct((count, width), BF), jax.ShapeDtypeStruct((count, width), F32), vec, vec),
        in_specs=[vmem, vmem, hbm, vmem, vmem],
        out_specs=(hbm, hbm, hbm, vmem, vmem),
        scratch_shapes=[pltpu.VMEM((count, depth), BF), pltpu.VMEM(w.shape, BF), pltpu.VMEM((count, width), F32), pltpu.VMEM((count, width), BF),
                        pltpu.VMEM((8, width), F32), pltpu.VMEM((8, width), F32), dma, dma, dma,
                        dma((2 * chips, 4)), dma((chips, 2)), dma, dma((4,)), dma((4,)), dma((count // TILE,))],
        compiler_params=pltpu.CompilerParams(collective_id=0, has_side_effects=True, vmem_limit_bytes=60 << 20),
        name='gather_layer',
    )(feat_a, feat_b, w, gain, bias)


def at_chunk(i):
    return pl.ds(pl.multiple_of(i * CHUNK, CHUNK), CHUNK)


def at_tile(i):
    return pl.ds(pl.multiple_of(i * TILE, TILE), TILE)


def any_spec():
    return pl.BlockSpec(memory_space=pl.ANY)


def now(j, tiles):
    return jnp.minimum(j, tiles - 1)


def past(j):
    return jnp.maximum(j - 1, 0)


def col_now(rows, tiles):
    return pl.BlockSpec((rows, TILE), lambda j: (0, now(j, tiles)))


def col_past(rows):
    return pl.BlockSpec((rows, TILE), lambda j: (0, past(j)))


def row_now(cols, tiles):
    return pl.BlockSpec((TILE, cols), lambda j: (now(j, tiles), 0))


def row_past(cols):
    return pl.BlockSpec((TILE, cols), lambda j: (past(j), 0))


def row_same(cols):
    return pl.BlockSpec((TILE, cols), lambda j: (j, 0))


def col_same(rows):
    return pl.BlockSpec((rows, TILE), lambda j: (0, j))


def params(**kw):
    return pltpu.CompilerParams(dimension_semantics=('arbitrary',), vmem_limit_bytes=60 << 20, **kw)


def cost(units):
    return pl.CostEstimate(flops=int(units * 2 * 2048 ** 3), bytes_accessed=40 << 20, transcendentals=0)


def row_load(src, dst, sem, i):
    return pltpu.make_async_copy(src.at[at_chunk(i), :], dst.at[at_chunk(i), :], sem.at[i])


def col_load(src, dst, sem, i):
    return pltpu.make_async_copy(src.at[:, at_chunk(i)], dst.at[:, at_chunk(i)], sem.at[i])


def row_sum(val):
    return jnp.sum(val, axis=0, keepdims=True)


def share(hold, other_ref, send_sem, recv_sem, t):
    return remote(hold.at[t], other_ref.at[:, at_tile(t)], send_sem.at[t], recv_sem.at[t], sibling_of(lax.axis_index(BATCH_AXIS)))


def layers_kernel(tiles, x_hbm, w_ref, g_ref, b_ref, w_last, act_ref, pre_ref, mean_ref, inv_ref, emb_ref, norm_ref, inv_last, other_ref,
                  x_ref, x_sem, act, pre, mean_s, inv_s, hold, send_sem, recv_sem):
    rows = x_ref.shape[0]
    chunks = rows // CHUNK
    step = pl.program_id(0)
    j = step - tiles - 1
    zero = (jnp.zeros((8, TILE), F32),) * 2

    def mul(left, right, i, sums):
        val = mm(left[at_chunk(i), :], right[...])
        pre[at_chunk(i), :] = val
        return sums[0] + fold(val), sums[1] + fold(val * val)

    def fin_layer(i):
        val = pre[at_chunk(i), :]
        pre_ref[at_chunk(i), :] = val
        norm = (val - mean_s[...]) * inv_s[...]
        new = jnp.maximum(norm * g_ref[...] + b_ref[...], 0.0).astype(BF)
        act_ref[at_chunk(i), :] = new
        act[at_chunk(i), at_tile(jnp.clip(step - 1, 0, tiles - 1))] = new

    def fin_last(i):
        norm = (pre[at_chunk(i), :] - mean_s[...]) * inv_s[...]
        norm_ref[at_chunk(i), :] = norm
        emb = norm.astype(BF)
        emb_ref[at_chunk(i), :] = emb
        hold[past(j), at_chunk(i), :] = emb

    def end(sums):
        mean = row_sum(sums[0]) / rows
        mean_s[...] = mean
        inv_s[...] = lax.rsqrt(row_sum(sums[1]) / rows - mean * mean + NORM_EPS)

    @pl.when(step == 0)
    def _():
        for i in range(chunks):
            row_load(x_hbm, x_ref, x_sem, i).start()
        greet([sibling_of(lax.axis_index(BATCH_AXIS))])

        def first(i, sums):
            row_load(x_hbm, x_ref, x_sem, i).wait()
            return mul(x_ref, w_ref, i, sums)
        end(lax.fori_loop(0, chunks, first, zero))

    @pl.when(jnp.logical_and(step > 0, step <= tiles))
    def _():
        mean_ref[...] = mean_s[...]
        inv_ref[...] = inv_s[...]

    @pl.when(j > 0)
    def _():
        inv_last[...] = inv_s[...]

    def both(fin, left, right):
        sums = zero
        for i in range(chunks):
            fin(i)
            sums = mul(left, right, i, sums)
        end(sums)

    def only(fin):
        def one(i, carry):
            fin(i)
            return carry
        lax.fori_loop(0, chunks, one, 0)

    @pl.when(jnp.logical_and(step > 0, step < tiles))
    def _():
        both(fin_layer, x_ref, w_ref)

    @pl.when(step == tiles)
    def _():
        only(fin_layer)

    @pl.when(j == 0)
    def _():
        end(lax.fori_loop(0, chunks, lambda i, sums: mul(act, w_last, i, sums), zero))

    @pl.when(jnp.logical_and(j > 0, j < tiles))
    def _():
        both(fin_last, act, w_last)

    @pl.when(j == tiles)
    def _():
        only(fin_last)
    copy = functools.partial(share, hold, other_ref, send_sem, recv_sem)

    @pl.when(j > 0)
    def _():
        copy(j - 1).start()

    @pl.when(j == tiles)
    def _():
        def last(t, carry):
            copy(t).wait()
            return carry
        lax.fori_loop(0, tiles, last, 0)


def layers(x, w, gain, bias, w_last):
    rows, width = x.shape[0], w.shape[1]
    tiles = width // TILE
    wide, tall, vec = jax.ShapeDtypeStruct((rows, width), BF), jax.ShapeDtypeStruct((rows, width), F32), jax.ShapeDtypeStruct((1, width), F32)
    dma = pltpu.SemaphoreType.DMA

    def col(height, first, offset):
        return pl.BlockSpec((height, TILE), lambda s: (0, jnp.clip(s - first * (tiles + 1) - offset, 0, tiles - 1)))
    return pl.pallas_call(
        functools.partial(layers_kernel, tiles), grid=(2 * tiles + 2,),
        out_shape=(wide, tall, vec, vec, wide, tall, vec, wide),
        in_specs=[any_spec(), col(w.shape[0], 0, 0), col(1, 0, 1), col(1, 0, 1), col(w_last.shape[0], 1, 0)],
        out_specs=(col(rows, 0, 1), col(rows, 0, 1), col(1, 0, 1), col(1, 0, 1), col(rows, 1, 1), col(rows, 1, 1), col(1, 1, 1), any_spec()),
        scratch_shapes=[pltpu.VMEM(x.shape, BF), dma((rows // CHUNK,)), pltpu.VMEM((rows, width), BF), pltpu.VMEM((rows, TILE), F32), pltpu.VMEM((1, TILE), F32), pltpu.VMEM((1, TILE), F32),
                        pltpu.VMEM((tiles, rows, TILE), BF), dma((tiles,)), dma((tiles,))],
        compiler_params=params(collective_id=1, has_side_effects=True), cost_estimate=cost(2), name='layers',
    )(x, w, gain, bias, w_last)


def corr_kernel(lam_ref, emb_ref, other_ref, norm_ref, inv_ref, dout_ref, loss_ref, grad_c, scr):
    j = pl.program_id(0)
    rows, width = other_ref.shape
    scale = 1.0 / rows
    lam = lam_ref[0]

    @pl.when(j == 0)
    def _():
        loss_ref[...] = jnp.zeros_like(loss_ref)

    def corr_step(i, loss):
        at = pl.ds(pl.multiple_of(i * CHUNK, CHUNK), CHUNK)
        corr = mm(emb_ref[...], other_ref[:, at], 0, 0) * scale
        row_id = lax.broadcasted_iota(jnp.int32, corr.shape, 0) + j * TILE
        col_id = lax.broadcasted_iota(jnp.int32, corr.shape, 1) + i * CHUNK
        on_diag = row_id == col_id
        miss = 1.0 - corr
        lam_corr = lam * corr
        grad_c[:, at] = jnp.where(on_diag, -2.0 * miss, 2.0 * lam_corr).astype(BF)
        return loss + fold(jnp.where(on_diag, miss * miss, lam_corr * corr))
    loss = lax.fori_loop(0, width // CHUNK, corr_step, jnp.zeros((8, CHUNK), F32), unroll=True)
    loss_ref[...] += loss

    def emb_step(i, carry):
        at = pl.ds(pl.multiple_of(i * CHUNK, CHUNK), CHUNK)
        val = mm(other_ref[at, :], grad_c[...], 1, 1) * scale
        scr[at, :] = val
        return carry[0] + fold(val), carry[1] + fold(val * norm_ref[at, :])
    zero = jnp.zeros((8, TILE), F32)
    tot, crs = lax.fori_loop(0, rows // CHUNK, emb_step, (zero, zero), unroll=True)
    mean_grad = jnp.sum(tot, axis=0, keepdims=True) / rows
    mean_cross = jnp.sum(crs, axis=0, keepdims=True) / rows
    inv = inv_ref[...]

    def fin(i, carry):
        at = pl.ds(pl.multiple_of(i * TILE, TILE), TILE)
        dout_ref[at, :] = (inv * (scr[at, :] - mean_grad - norm_ref[at, :] * mean_cross)).astype(BF)
        return carry
    lax.fori_loop(0, rows // TILE, fin, 0)


def corr_back(lam_off, emb, other, norm, inv):
    rows, width = emb.shape
    return pl.pallas_call(
        corr_kernel, grid=(width // TILE,),
        out_shape=(jax.ShapeDtypeStruct((rows, width), BF), jax.ShapeDtypeStruct((8, CHUNK), F32)),
        in_specs=[pl.BlockSpec(memory_space=pltpu.SMEM), col_same(rows), pl.BlockSpec(other.shape, lambda j: (0, 0), pipeline_mode=pl.Buffered(1)), col_same(rows), col_same(1)],
        out_specs=(col_same(rows), pl.BlockSpec((8, CHUNK), lambda j: (0, 0))),
        scratch_shapes=[pltpu.VMEM((TILE, width), BF), pltpu.VMEM((rows, TILE), F32)],
        compiler_params=params(), cost_estimate=cost(2), name='corr_back',
    )(lam_off.reshape(1), emb, other, norm, inv)


def back_kernel(tiles, layered, act_hbm, d_hbm, *refs):
    if layered:
        w_ref, pre_ref, mean_ref, scale_ref, inv_ref, g_ref, b_ref, g_old, dpre_ref, dg_ref, db_ref, dw_out = refs[:12]
        d_ref, d_sem, lhs, lhs_sem, sbuf, rbuf, ps, pr, os_, or_, ol, scr, norm_s, grad_s, cross_s = refs[12:]
    else:
        vecs, loss_ref, dw_out, small_out = refs[:4], refs[4], refs[5], refs[6]
        d_ref, d_sem, lhs, lhs_sem, sbuf, rbuf, ps, pr, os_, or_, ol, small_ref, small_in, ss, sr = refs[7:]
    step = pl.program_id(0)
    rows, width = d_ref.shape
    half = sbuf.shape[0]
    chunks = width // CHUNK
    me = lax.axis_index(BATCH_AXIS)
    core = lax.rem(me, 2)
    sib = sibling_of(me)
    after = step - half
    if layered:
        turn, place = after // 3, lax.rem(after, 3)
        own_turn = jnp.logical_and(jnp.logical_and(after >= 0, after < 3 * half), place == 1)
        tile_turn = jnp.logical_and(jnp.logical_and(after >= 0, after < 3 * half), place != 1)
        last_step = 3 * half
    else:
        turn = after
        own_turn = after >= 0
        last_step = half - 1

    def load_left(q):
        mine = q // half
        tile = (mine * core + (1 - mine) * (1 - core)) * half + q - mine * half
        return pltpu.make_async_copy(act_hbm.at[:, at_tile(tile)], lhs.at[lax.rem(q, 2)], lhs_sem.at[lax.rem(q, 2)])

    def part_copy(t):
        return remote(sbuf.at[t], rbuf.at[t], ps.at[t], pr.at[t], sib)

    def result_rows(t):
        return dw_out.at[at_tile(core * half + t), :]

    def sum_copy(t):
        return remote(sbuf.at[t], result_rows(t), os_.at[t], or_.at[t], sib)

    def own_copy(t):
        return pltpu.make_async_copy(sbuf.at[t], result_rows(t), ol.at[t])

    def load_d(i):
        return col_load(d_hbm, d_ref, d_sem, i)

    def product(q, i):
        return mm(lhs[lax.rem(q, 2)], d_ref[:, at_chunk(i)], 0, 0)

    @pl.when(step == 0)
    def _():
        load_left(0).start()
        for i in range(chunks):
            load_d(i).start()
        load_left(1).start()
        greet([sib])
        if not layered:
            small_ref[...] = jnp.zeros_like(small_ref)
            for k, vec in enumerate(vecs):
                small_ref[k:k + 1, :] = vec[...]
            small_ref[4:5, :] = jnp.zeros((1, width), F32) + jnp.where(core == 0, jnp.sum(loss_ref[...]), 0.0)
        load_left(0).wait()

        def first(i, carry):
            load_d(i).wait()
            sbuf[0, :, at_chunk(i)] = product(0, i)
            return carry
        lax.fori_loop(0, chunks, first, 0)
        part_copy(0).start()

    @pl.when(jnp.logical_and(step > 0, step < half))
    def _():
        load_left(step + 1).start()
        load_left(step).wait()
        for i in range(chunks):
            sbuf[step, :, at_chunk(i)] = product(step, i)
        part_copy(step).start()
        if not layered:
            @pl.when(step == 1)
            def _():
                remote(small_ref, small_in, ss, sr, sib).start()

    if layered:
        def mul(i, sums):
            val = mm(d_ref[at_chunk(i), :], w_ref[...], 1, 1)
            norm = (pre_ref[at_chunk(i), :] - mean_ref[...]) * scale_ref[...]
            val = jnp.where(norm * g_ref[...] + b_ref[...] > 0, val, 0.0)
            scr[at_chunk(i), :] = val
            norm_s[at_chunk(i), :] = norm
            return sums[0] + fold(val), sums[1] + fold(val * norm)

        def fin(i):
            dpre_ref[at_chunk(i), :] = (inv_ref[...] * (scr[at_chunk(i), :] * g_old[...] - grad_s[...] - norm_s[at_chunk(i), :] * cross_s[...])).astype(BF)
        zero = (jnp.zeros((8, TILE), F32),) * 2

        @pl.when(tile_turn)
        def _():
            sums = zero
            for i in range(rows // CHUNK):
                fin(i)
                sums = mul(i, sums)
            tot, crs = row_sum(sums[0]), row_sum(sums[1])
            db_ref[...] = tot
            dg_ref[...] = crs
            grad_s[...] = g_ref[...] * tot / rows
            cross_s[...] = g_ref[...] * crs / rows

        @pl.when(after == last_step)
        def _():
            def last(i, carry):
                fin(i)
                return carry
            lax.fori_loop(0, rows // CHUNK, last, 0)

    @pl.when(own_turn)
    def _():
        t = turn
        q = t + half

        @pl.when(t + 1 < half)
        def _():
            load_left(q + 1).start()
        load_left(q).wait()
        part_copy(t).wait()
        for i in range(chunks):
            sbuf[t, :, at_chunk(i)] = product(q, i) + rbuf[t, :, at_chunk(i)]
        sum_copy(t).start()
        own_copy(t).start()

    @pl.when(after == last_step)
    def _():
        def end(k, carry):
            sum_copy(k).wait()
            own_copy(k).wait()
            return carry
        lax.fori_loop(0, half, end, 0)
        if not layered:
            remote(small_ref, small_in, ss, sr, sib).wait()
            small_out[...] = small_ref[...] + small_in[...]


def layer_back(ident, act, grad, layer_args=None, small=None):
    rows, width = grad.shape
    depth = act.shape[1]
    half = depth // TILE // 2
    dma = pltpu.SemaphoreType.DMA
    hbm = any_spec()
    scratch = [pltpu.VMEM(grad.shape, BF), dma((width // CHUNK,)), pltpu.VMEM((2, rows, TILE), BF), dma((2,)), pltpu.VMEM((half, TILE, width), F32),
               pltpu.VMEM((half, TILE, width), F32)] + [dma((half,))] * 5
    dw = jax.ShapeDtypeStruct((depth, width), F32)
    if layer_args is not None:
        w, pre, mean, scale, inv, gain, bias = layer_args
        tiles = w.shape[0] // TILE

        def cur(s):
            return jnp.clip((2 * jnp.maximum(s - half, 0) + 1) // 3, 0, tiles - 1)

        def old(s):
            return jnp.clip((2 * jnp.maximum(s - half, 0) + 1) // 3 - 1, 0, tiles - 1)
        vec_cur = pl.BlockSpec((1, TILE), lambda s: (0, cur(s)))
        vec_old = pl.BlockSpec((1, TILE), lambda s: (0, old(s)))
        in_specs = [hbm, hbm, pl.BlockSpec((TILE, w.shape[1]), lambda s: (cur(s), 0)), pl.BlockSpec((rows, TILE), lambda s: (0, cur(s))),
                    vec_cur, vec_cur, vec_old, vec_cur, vec_cur, vec_old]
        out_specs = (pl.BlockSpec((rows, TILE), lambda s: (0, old(s))), vec_cur, vec_cur, hbm)
        vec = jax.ShapeDtypeStruct((1, depth), F32)
        out_shape = (jax.ShapeDtypeStruct((rows, depth), BF), vec, vec, dw)
        scratch += [pltpu.VMEM((rows, TILE), F32), pltpu.VMEM((rows, TILE), F32), pltpu.VMEM((1, TILE), F32), pltpu.VMEM((1, TILE), F32)]
        args = (act, grad, w, pre, mean, scale, inv, gain, bias, gain)
        steps = 2 * half + tiles + 1
    else:
        tiles = 0
        in_specs = [hbm, hbm] + [pl.BlockSpec(v.shape, lambda s: (0, 0)) for v in small]
        out_specs = (hbm, pl.BlockSpec((8, width), lambda s: (0, 0)))
        out_shape = (dw, jax.ShapeDtypeStruct((8, width), F32))
        scratch += [pltpu.VMEM((8, width), F32), pltpu.VMEM((8, width), F32), dma, dma]
        args = (act, grad, *small)
        steps = 2 * half
    return pl.pallas_call(
        functools.partial(back_kernel, tiles, layer_args is not None), grid=(steps,),
        out_shape=out_shape, in_specs=in_specs, out_specs=out_specs, scratch_shapes=scratch,
        compiler_params=params(collective_id=ident, has_side_effects=True), cost_estimate=cost(2), name='back_%d' % ident,
    )(*args)


def solution(mesh):
    num_devs = mesh.shape[BATCH_AXIS]

    def local_step(feat_a, feat_b, w_one, w_two, w_three, g_one, b_one, g_two, b_two, lam_off):
        g_one, b_one, g_two, b_two = (v.reshape(1, -1) for v in (g_one, b_one, g_two, b_two))
        feat, act_one, pre_one, mean_one, inv_one = gather_layer(feat_a, feat_b, w_one, g_one, b_one, num_devs)
        act_two, pre_two, mean_two, inv_two, emb, norm_out, inv_out, other = layers(act_one, w_two, g_two, b_two, w_three)
        grad_out, loss = corr_back(lam_off, emb, other, norm_out, inv_out)
        grad_two, dg_two, db_two, dw_three = layer_back(2, act_two, grad_out, (w_three, pre_two, mean_two, inv_two, inv_two, g_two, b_two))
        grad_one, dg_one, db_one, dw_two = layer_back(3, act_one, grad_two, (w_two, pre_one, mean_one, inv_one, inv_one, g_one, b_one))
        dw_one, small = layer_back(4, feat, grad_one, small=(dg_one, db_one, dg_two, db_two, loss))
        return (small[4, 0], dw_one, dw_two, dw_three, small[0], small[1], small[2], small[3])

    row_spec = P(BATCH_AXIS, None)
    return jax.shard_map(local_step, mesh=mesh, in_specs=(row_spec, row_spec, P(), P(), P(), P(), P(), P(), P(), P()), out_specs=(P(), P(), P(), P(), P(), P(), P(), P()), check_vma=False)
```
